16 devices in a mesh: dp: 2 (over y, z), ep: 8 (over x, core).
Axes of the slice: x: 4, y: 2, z: 1, core: 2. Of those that a mesh axis runs over, the one named last changes fastest.
The devices are a block of a 4x4x8 slice.
Arguments:
- h0: bfloat16 [16, 1024, 2048], P(('dp', 'ep')), parts along dimension 0
- idx: int32 [16, 1024, 6], P(('dp', 'ep')), parts along dimension 0
- slot: int32 [16, 1024, 6], P(('dp', 'ep')), parts along dimension 0
- norm_attn: bfloat16 [2048], replicated
- wq: bfloat16 [2048, 2048], replicated
- wk: bfloat16 [2048, 2048], replicated
- wv: bfloat16 [2048, 2048], replicated
- wo: bfloat16 [2048, 2048], replicated
- norm_ffn: bfloat16 [2048], replicated
- w1: bfloat16 [2048, 10944], replicated
- w3: bfloat16 [2048, 10944], replicated
- w2: bfloat16 [10944, 2048], replicated
- norm_moe: bfloat16 [2048], replicated
- wr: bfloat16 [2048, 64], replicated
- ue1: bfloat16 [64, 2048, 1408], P('ep')
- ue3: bfloat16 [64, 2048, 1408], P('ep')
- ue2: bfloat16 [64, 1408, 2048], P('ep')
Outputs:
- output: bfloat16 [16, 1024, 2048], P(('dp', 'ep')), parts along dimension 0
There are 2 independent parts. The reference program is written for one: setup_inputs(seed, part) draws one part's arguments, and reference() takes and returns one part's arrays. A program takes and returns all parts, laid end to end along the dimension named above; an argument that names none is the same for every part.
All inputs are finite; a program needn't handle non-finite values.
Results may differ from the reference program's by a relative error of at most 0.00946092.
Values are sent between devices in bfloat16 or wider.
A program may use at most 768 MiB of HBM per device.

```python
import jax
import jax.numpy as jnp
from jax import lax

D = 2048
HEADS = 16
KV_HEADS = 16
HEAD = 128
FF = 10944
EXPERTS = 64
TOP = 6
FE = 1408
SEQS_DEV = 1
SEQ = 1024
EP = 8

TOKENS = SEQS_DEV * SEQ
CAP = 2 * TOKENS * TOP // EXPERTS
EPS = 1e-6
ROPE_BASE = 10000.0


def _w(key, shape, fan_in, scale=1.0):
    return (scale * fan_in ** -0.5 * jax.random.normal(key, shape, jnp.float32)).astype(jnp.bfloat16)


def _perms(key, count, size):
    return jax.vmap(lambda k: jax.random.permutation(k, size))(jax.random.split(key, count))


def setup_inputs(seed: int = 0, part: int = 0) -> dict:
    key = jax.random.PRNGKey(seed)
    ks = jax.random.split(key, 14)
    kp = jax.random.split(jax.random.fold_in(key, part), 4)
    kd = jax.random.split(jax.random.fold_in(jax.random.fold_in(key, part), 7), 4)
    avg = TOKENS * TOP // EXPERTS
    c = jnp.arange(TOKENS * TOP).reshape(TOKENS, TOP)
    half = TOKENS * TOP // 2
    low = c < half
    e0 = jnp.where(low, c % EXPERTS, (c - half) % (EXPERTS // 2))
    s0 = jnp.where(low, c // EXPERTS, avg // 2 + (c - half) // (EXPERTS // 2))
    shift = jax.random.randint(kd[2], (EP, EXPERTS), 0, CAP)
    tperm = jnp.broadcast_to(_perms(kd[3], EP, TOKENS)[:, :, None], (EP, TOKENS, TOP))
    idx = jnp.take_along_axis(jnp.broadcast_to(e0, (EP, TOKENS, TOP)), tperm, axis=1)
    slot = jnp.take_along_axis((s0[None] + shift[:, e0]) % CAP, tperm, axis=1)
    rshape = (EP * SEQS_DEV, SEQ, TOP)

    def nrm(k):
        return (1.0 + 0.2 * jax.random.normal(k, (D,), jnp.float32)).astype(jnp.bfloat16)

    return {
        'h0': jax.random.normal(kp[0], (EP * SEQS_DEV, SEQ, D), jnp.float32).astype(jnp.bfloat16),
        'idx': idx.reshape(rshape).astype(jnp.int32),
        'slot': slot.reshape(rshape).astype(jnp.int32),
        'norm_attn': nrm(ks[0]),
        'wq': _w(ks[1], (D, HEADS * HEAD), D),
        'wk': _w(ks[2], (D, KV_HEADS * HEAD), D),
        'wv': _w(ks[3], (D, KV_HEADS * HEAD), D),
        'wo': _w(ks[4], (HEADS * HEAD, D), HEADS * HEAD, 2.0),
        'norm_ffn': nrm(ks[5]),
        'w1': _w(ks[6], (D, FF), D),
        'w3': _w(ks[7], (D, FF), D),
        'w2': _w(ks[8], (FF, D), FF, 2.0),
        'norm_moe': nrm(ks[9]),
        'wr': _w(ks[10], (D, EXPERTS), D, 2.0),
        'ue1': _w(ks[11], (EXPERTS, D, FE), D),
        'ue3': _w(ks[12], (EXPERTS, D, FE), D),
        'ue2': _w(ks[13], (EXPERTS, FE, D), FE, 2.0),
    }


def _rms(x, w):
    xf = x.astype(jnp.float32)
    r = lax.rsqrt(jnp.mean(xf * xf, axis=-1, keepdims=True) + EPS)
    return (xf * r * w.astype(jnp.float32)).astype(jnp.bfloat16)


def _rope(x, cos, sin):
    h = HEAD // 2
    x1 = x[..., :h]
    x2 = x[..., h:]
    return jnp.concatenate([x1 * cos - x2 * sin, x2 * cos + x1 * sin], axis=-1)


def _dense_seq(h, na, wq, wk, wv, wo, nf, w1, w3, w2):
    f32 = jnp.float32
    bf = jnp.bfloat16
    pos = jnp.arange(SEQ).astype(f32)
    inv = ROPE_BASE ** (-2.0 * jnp.arange(HEAD // 2).astype(f32) / HEAD)
    ang = pos[:, None] * inv[None, :]
    cos = jnp.cos(ang)[:, None, :]
    sin = jnp.sin(ang)[:, None, :]
    x = _rms(h, na)
    q = _rope(jnp.dot(x, wq, preferred_element_type=f32).reshape(SEQ, HEADS, HEAD), cos, sin).astype(bf)
    k = _rope(jnp.dot(x, wk, preferred_element_type=f32).reshape(SEQ, KV_HEADS, HEAD), cos, sin).astype(bf)
    v = jnp.dot(x, wv, preferred_element_type=f32).astype(bf).reshape(SEQ, KV_HEADS, HEAD)
    q = q.reshape(SEQ, KV_HEADS, HEADS // KV_HEADS, HEAD)
    s = jnp.einsum('qgrd,kgd->grqk', q.astype(f32), k.astype(f32)) * HEAD ** -0.5
    causal = jnp.arange(SEQ)[:, None] >= jnp.arange(SEQ)[None, :]
    s = jnp.where(causal, s, -jnp.inf)
    p = jax.nn.softmax(s, axis=-1).astype(bf)
    o = jnp.einsum('grqk,kgd->qgrd', p.astype(f32), v.astype(f32)).astype(bf).reshape(SEQ, HEADS * HEAD)
    a = (h.astype(f32) + jnp.dot(o, wo, preferred_element_type=f32)).astype(bf)
    z = _rms(a, nf)
    hid = (jax.nn.silu(jnp.dot(z, w1, preferred_element_type=f32)) * jnp.dot(z, w3, preferred_element_type=f32)).astype(bf)
    return a.astype(f32) + jnp.dot(hid, w2, preferred_element_type=f32)


def reference(h0, idx, slot, norm_attn, wq, wk, wv, wo, norm_ffn, w1, w3, w2, norm_moe, wr, ue1, ue3, ue2):
    f32 = jnp.float32
    bf = jnp.bfloat16
    n = EP * TOKENS
    ix = idx.reshape(n, TOP)
    sl = slot.reshape(n, TOP)
    u = _rms(h0.reshape(n, D), norm_moe)
    logits = jnp.dot(u, wr, preferred_element_type=f32)
    g = jax.nn.softmax(jnp.take_along_axis(logits, ix, axis=1), axis=-1)
    rows = jnp.broadcast_to(jnp.arange(n, dtype=jnp.int32)[:, None], (n, TOP))
    src = rows // TOKENS
    tok = jnp.full((EP, EXPERTS, CAP), n, jnp.int32).at[src, ix, sl].set(rows)
    gb = jnp.zeros((EP, EXPERTS, CAP), f32).at[src, ix, sl].set(g)
    tok = tok.transpose(1, 0, 2).reshape(EXPERTS, EP * CAP)
    x = jnp.take(u, tok, axis=0, mode='fill', fill_value=0)

    def expert(args):
        xe, e1, e3, e2 = args
        hid = (jax.nn.silu(jnp.dot(xe, e1, preferred_element_type=f32)) * jnp.dot(xe, e3, preferred_element_type=f32)).astype(bf)
        return jnp.dot(hid, e2, preferred_element_type=f32).astype(bf)

    y = lax.map(expert, (x, ue1, ue3, ue2))
    gw = gb.transpose(1, 0, 2).reshape(EXPERTS, EP * CAP, 1)
    m = jnp.zeros((n, D), f32).at[tok.reshape(-1)].add((gw * y.astype(f32)).reshape(-1, D), mode='drop')
    dense = lax.map(lambda hs: _dense_seq(hs, norm_attn, wq, wk, wv, wo, norm_ffn, w1, w3, w2), h0)
    return (dense + m.reshape(EP * SEQS_DEV, SEQ, D)).astype(bf)
```

```python
import functools

import jax
import jax.numpy as jnp
from jax import lax
from jax.experimental import pallas as pl
from jax.experimental.pallas import tpu as pltpu
from jax.sharding import PartitionSpec as P

HEAD = 128
EPS = 1e-6
ROPE_BASE = 10000.0
CHUNKS = 2
GR = 16
BG = 256
BM = 384
TB = 128
WIN = 64
F32, BF = jnp.float32, jnp.bfloat16


def _rms(x, w):
    xf = x.astype(F32)
    r = lax.rsqrt(jnp.mean(xf * xf, axis=-1, keepdims=True) + EPS)
    return (xf * r * w.astype(F32)).astype(BF)


def _attn_kernel(scale, qb, q_ref, k_ref, v_ref, cos_ref, sin_ref, o_ref):
    cos, sin = cos_ref[...], sin_ref[...]
    half = HEAD // 2

    def rope(x):
        return (x * cos + pltpu.roll(x, half, 1) * sin).astype(BF)

    q, k, v = rope(q_ref[...]), rope(k_ref[...]), v_ref[...]
    n = q.shape[0] // qb
    for i in range(n):
        kv = (i + 1) * qb
        s = lax.dot_general(q[i * qb:(i + 1) * qb], k[:kv], (((1,), (1,)), ((), ())),
                            preferred_element_type=F32) * scale
        row = lax.broadcasted_iota(jnp.int32, (qb, kv), 0) + i * qb
        col = lax.broadcasted_iota(jnp.int32, (qb, kv), 1)
        s = jnp.where(row >= col, s, -jnp.inf)
        p = jnp.exp(s - jnp.max(s, axis=-1, keepdims=True))
        p = (p / jnp.sum(p, axis=-1, keepdims=True)).astype(BF)
        o = jnp.dot(p, v[:kv], preferred_element_type=F32)
        o_ref[i * qb:(i + 1) * qb, :] = o.astype(BF)


def _attention(q, k, v, cos, sin):
    s, dq = q.shape
    blk = pl.BlockSpec((s, HEAD), lambda h: (0, h))
    tab = pl.BlockSpec((s, HEAD), lambda h: (0, 0))
    return pl.pallas_call(
        functools.partial(_attn_kernel, HEAD ** -0.5, min(256, s)),
        out_shape=jax.ShapeDtypeStruct((s, dq), BF),
        grid=(dq // HEAD,),
        in_specs=[blk, blk, blk, tab, tab],
        out_specs=blk,
        compiler_params=pltpu.CompilerParams(vmem_limit_bytes=40 * 2**20),
        cost_estimate=pl.CostEstimate(flops=4 * s * s * dq, bytes_accessed=12 * s * dq, transcendentals=s * s * dq // HEAD),
        name="attention",
    )(q, k, v, cos, sin)


def _gather_kernel(ng, ge, gr0, gdst, stot, u_ref, rk_ref, x_hbm, xbuf, sem):
    s = pl.program_id(0)
    tc = u_ref.shape[0]
    per = BG // GR
    total = stot[s]
    iota = lax.broadcasted_iota(jnp.int32, (GR, tc), 0)

    def copies(m, act):
        slot = lax.rem(m, 2)
        for k in range(per):
            g = m * per + k

            @pl.when(g < total)
            def _():
                act(pltpu.make_async_copy(
                    xbuf.at[slot, pl.ds(k * GR, GR), :],
                    x_hbm.at[pl.ds(pl.multiple_of(gdst[s, g] * GR, GR), GR), :],
                    sem.at[slot, k]))

    def tile(m, _):
        @pl.when(m >= 2)
        def _():
            copies(m - 2, lambda c: c.wait())

        parts = []
        for k in range(per):
            g = m * per + k
            row = rk_ref[0, pl.ds(ge[s, g], 1), :]
            pos = iota + gr0[s, g]
            parts.append((pos.astype(F32) == row).astype(F32).astype(BF))
        onehot = jnp.concatenate(parts, axis=0)
        xbuf[lax.rem(m, 2)] = jnp.dot(onehot, u_ref[...], preferred_element_type=F32).astype(BF)
        copies(m, lambda c: c.start())
        return 0

    tiles = lax.div(total + per - 1, per)
    lax.fori_loop(0, tiles, tile, 0)

    @pl.when(tiles >= 2)
    def _():
        copies(tiles - 2, lambda c: c.wait())

    @pl.when(tiles >= 1)
    def _():
        copies(tiles - 1, lambda c: c.wait())


def _gather(u, rk, tabs, rows, ng):
    srcs, el, tc = rk.shape
    d = u.shape[1]
    return pl.pallas_call(
        functools.partial(_gather_kernel, ng),
        out_shape=jax.ShapeDtypeStruct((rows, d), BF),
        grid_spec=pltpu.PrefetchScalarGridSpec(
            num_scalar_prefetch=4,
            grid=(srcs,),
            in_specs=[pl.BlockSpec((tc, d), lambda s, *_: (s, 0)),
                      pl.BlockSpec((1, el, tc), lambda s, *_: (s, 0, 0))],
            out_specs=pl.BlockSpec(memory_space=pl.ANY),
            scratch_shapes=[pltpu.VMEM((2, BG, d), BF), pltpu.SemaphoreType.DMA((2, BG // GR))],
        ),
        compiler_params=pltpu.CompilerParams(vmem_limit_bytes=48 * 2**20),
        cost_estimate=pl.CostEstimate(flops=2 * rows * tc * d, bytes_accessed=4 * rows * d, transcendentals=0),
        name="gather_rows",
    )(*tabs, u, rk)


def _expert_kernel(te, tv, nt, x_ref, w1_ref, w3_ref, w2_ref, y_ref):
    i = pl.program_id(0)

    @pl.when(i < nt[0])
    def _():
        x = x_ref[...]
        h1 = jnp.dot(x, w1_ref[0], preferred_element_type=F32)
        h3 = jnp.dot(x, w3_ref[0], preferred_element_type=F32)
        hid = (jax.nn.silu(h1) * h3).astype(BF)
        y = jnp.dot(hid, w2_ref[0], preferred_element_type=F32)
        row = lax.broadcasted_iota(jnp.int32, (y.shape[0], 1), 0)
        y_ref[...] = jnp.where(row < tv[i], y, 0.0).astype(BF)


def _experts(x, ue1, ue3, ue2, te, tv, nt, max_tiles):
    el, d, fe = ue1.shape

    def rowmap(i, te, tv, nt):
        return (jnp.minimum(i, nt[0] - 1), 0)

    def wmap(i, te, tv, nt):
        return (te[i], 0, 0)

    rows = max_tiles * BM
    return pl.pallas_call(
        _expert_kernel,
        out_shape=jax.ShapeDtypeStruct((rows, d), BF),
        grid_spec=pltpu.PrefetchScalarGridSpec(
            num_scalar_prefetch=3,
            grid=(max_tiles,),
            in_specs=[pl.BlockSpec((BM, d), rowmap),
                      pl.BlockSpec((1, d, fe), wmap),
                      pl.BlockSpec((1, d, fe), wmap),
                      pl.BlockSpec((1, fe, d), wmap)],
            out_specs=pl.BlockSpec((BM, d), rowmap),
        ),
        compiler_params=pltpu.CompilerParams(vmem_limit_bytes=61 * 2**20),
        cost_estimate=pl.CostEstimate(flops=3 * rows * d * fe, bytes_accessed=6 * el * d * fe, transcendentals=rows * fe),
        name="experts",
    )(te, tv, nt, x, ue1, ue3, ue2)


def _combine_kernel(nb, st, tend, nwin, y_hbm, pos_ref, g_ref, o_ref, ybuf, sem):
    s, b = pl.program_id(0), pl.program_id(1)
    el = pos_ref.shape[1]
    i = s * nb + b
    last = pl.num_programs(0) * nb - 1
    slot = lax.rem(i, 2)

    def start_of(step, e, w):
        return jnp.minimum(st[step, e] + w * WIN, tend[e] - WIN)

    def windows(step, w, sl, act):
        for e in range(el):
            act(pltpu.make_async_copy(
                y_hbm.at[pl.ds(pl.multiple_of(start_of(step, e, w), GR), WIN), :],
                ybuf.at[sl, pl.ds(e * WIN, WIN), :],
                sem.at[sl, e]))

    @pl.when(i == 0)
    def _():
        windows(0, 0, 0, lambda c: c.start())

    @pl.when(i < last)
    def _():
        windows(i + 1, 0, 1 - slot, lambda c: c.start())

    gates = g_ref[0]
    g1 = gates.astype(BF).astype(F32)
    r1 = gates - g1
    g2 = r1.astype(BF).astype(F32)
    terms = (g1, g2, r1 - g2)
    iota = lax.broadcasted_iota(jnp.int32, (WIN, TB), 0)

    def part(w, sl):
        cols = []
        for term in terms:
            rows = []
            for e in range(el):
                pos = pos_ref[0, e:e + 1, :]
                lo = st[i, e] + w * WIN
                ok = (pos >= lo) & (pos < lo + WIN)
                rel = jnp.where(ok, pos - start_of(i, e, w), -1)
                rows.append(jnp.where(iota == rel, term[e:e + 1, :], 0.0).astype(BF))
            cols.append(jnp.concatenate(rows, axis=0))
        wt = jnp.concatenate(cols, axis=1)
        r = lax.dot_general(wt, ybuf[sl], (((0,), (0,)), ((), ())), preferred_element_type=F32)
        return r[:TB] + r[TB:2 * TB] + r[2 * TB:]

    windows(i, 0, slot, lambda c: c.wait())
    o_ref[...] = part(0, slot)

    def more(w, _):
        windows(i, w, 2, lambda c: c.start())
        windows(i, w, 2, lambda c: c.wait())
        o_ref[...] += part(w, 2)
        return 0

    lax.fori_loop(1, nwin[i], more, 0)


def _combine(y, pos, gate, st, tend, nwin):
    srcs, el, tc = pos.shape
    d = y.shape[1]
    nb = tc // TB
    blk = pl.BlockSpec((1, el, TB), lambda s, b, *_: (s, 0, b))
    return pl.pallas_call(
        functools.partial(_combine_kernel, nb),
        out_shape=jax.ShapeDtypeStruct((srcs * tc, d), F32),
        grid_spec=pltpu.PrefetchScalarGridSpec(
            num_scalar_prefetch=3,
            grid=(srcs, nb),
            in_specs=[pl.BlockSpec(memory_space=pl.ANY), blk, blk],
            out_specs=pl.BlockSpec((TB, d), lambda s, b, *_: (s * nb + b, 0)),
            scratch_shapes=[pltpu.VMEM((3, el * WIN, d), BF), pltpu.SemaphoreType.DMA((3, el))],
        ),
        compiler_params=pltpu.CompilerParams(vmem_limit_bytes=48 * 2**20),
        cost_estimate=pl.CostEstimate(flops=6 * srcs * tc * el * WIN * d, bytes_accessed=4 * srcs * tc * d, transcendentals=0),
        name="combine",
    )(st, tend, nwin, y, pos, gate)


def _excl(x, axis):
    return jnp.cumsum(x, axis=axis) - x


def _tables(rk, cap):
    srcs, el, tc = rk.shape
    i32 = jnp.int32
    nb = tc // TB
    has = (rk >= 0).reshape(srcs, el, nb, TB).sum(-1, dtype=i32)
    hi = jnp.cumsum(has, axis=2)
    lo = hi - has
    gran = (hi[:, :, -1] + GR - 1) // GR
    tot = gran.sum(0)
    tiles = jnp.maximum(1, (tot * GR + BM - 1) // BM)
    tbase = _excl(tiles, 0)
    seg = tbase * (BM // GR) + _excl(gran, 0)
    soff = _excl(gran, 1)
    stot = gran.sum(1)
    ng = el * (cap // GR + (cap % GR > 0)) + BG // GR
    gi = jnp.arange(ng, dtype=i32)
    own = (gi[None, :, None] >= soff[:, None, :]) & (gi[None, :, None] < (soff + gran)[:, None, :])
    eid = jnp.arange(el, dtype=i32)
    ge = jnp.sum(jnp.where(own, eid, 0), -1)
    live = gi[None, :] < stot[:, None]
    gr0 = jnp.where(live, gi[None, :] - jnp.sum(jnp.where(own, soff[:, None, :], 0), -1), 1 << 16) * GR
    gdst = jnp.sum(jnp.where(own, (seg - soff)[:, None, :], 0), -1) + gi[None, :]
    max_tiles = el * (-(-(srcs * (-(-cap // GR)) * GR) // BM))
    nt = tiles.sum()
    ti = jnp.arange(max_tiles, dtype=i32)
    te = jnp.sum((ti[:, None] >= (tbase + tiles)[None, :]).astype(i32), -1)
    te = jnp.minimum(te, el - 1)
    mine = te[:, None] == eid[None, :]
    tv = jnp.sum(jnp.where(mine, (tot * GR + tbase * BM)[None, :], 0), -1) - ti * BM
    tend = (tbase + tiles) * BM
    lo16 = lo // GR * GR
    st = (lo16 + seg[:, :, None] * GR).transpose(0, 2, 1).reshape(srcs * nb, el)
    nwin = jnp.max((hi - lo16 + WIN - 1) // WIN, axis=1).reshape(srcs * nb)
    pos = jnp.where(rk >= 0, rk.astype(i32) + seg[:, :, None] * GR, -1)
    return (ge, gr0, gdst, stot), (te, tv, nt.reshape(1)), (st, tend, nwin), pos, max_tiles, ng


def solution(mesh):
    G = mesh.shape['ep']

    def local(h0, idx, slot, na, wq, wk, wv, wo, nf, w1, w3, w2, nm, wr, ue1, ue3, ue2):
        b, s, d = h0.shape
        t = b * s
        k = idx.shape[-1]
        el = ue1.shape[0]
        e = el * G
        cap = 2 * t * k // e
        tc = t // CHUNKS
        h = h0.reshape(t, d)

        u = _rms(h, nm)
        us = [lax.all_gather(u[c * tc:(c + 1) * tc], 'ep', axis=0, tiled=True) for c in range(CHUNKS)]

        idxt = idx.reshape(t, k).T
        hit = (idxt[:, None, :] == jnp.arange(e, dtype=jnp.int32)[None, :, None]).any(0)
        logits = lax.dot_general(wr, u, (((0,), (1,)), ((), ())), preferred_element_type=F32)
        top = jnp.max(jnp.where(hit, logits, -jnp.inf), axis=0, keepdims=True)
        ex = jnp.where(hit, jnp.exp(logits - top), 0.0)
        gate = ex / jnp.sum(ex, axis=0, keepdims=True)
        before = (jnp.arange(tc)[:, None] < jnp.arange(tc)[None, :]).astype(BF)
        rank = jnp.dot(hit.astype(BF).reshape(e * CHUNKS, tc), before, preferred_element_type=F32).reshape(e, t)
        rank = jnp.where(hit, rank, -1.0)
        route = jnp.concatenate([rank.reshape(G, el, t), gate.reshape(G, el, t)], axis=1)
        route = lax.all_to_all(route, 'ep', 0, 0, tiled=True)

        pos = jnp.arange(s).astype(F32)
        inv = ROPE_BASE ** (-2.0 * jnp.arange(HEAD // 2).astype(F32) / HEAD)
        ang = pos[:, None] * inv[None, :]
        cos, sin = jnp.cos(ang), jnp.sin(ang)
        cosf = jnp.concatenate([cos, cos], axis=1)
        sinf = jnp.concatenate([-sin, sin], axis=1)
        x = _rms(h, na)
        q = jnp.dot(x, wq, preferred_element_type=F32)
        kk = jnp.dot(x, wk, preferred_element_type=F32)
        v = jnp.dot(x, wv, preferred_element_type=F32).astype(BF)
        o = jnp.concatenate([_attention(q[i * s:(i + 1) * s], kk[i * s:(i + 1) * s], v[i * s:(i + 1) * s], cosf, sinf)
                             for i in range(b)], axis=0)
        a = (h.astype(F32) + jnp.dot(o, wo, preferred_element_type=F32)).astype(BF)

        ms = []
        gatekeeper = a
        for c in range(CHUNKS):
            rk = route[:, :el, c * tc:(c + 1) * tc]
            gt = route[:, el:, c * tc:(c + 1) * tc]
            gtab, etab, ctab, ps, max_tiles, ng = _tables(rk, cap)
            uc, gatekeeper = lax.optimization_barrier((us[c], gatekeeper))
            xr = _gather(uc, rk, gtab, max_tiles * BM, ng)
            y = _experts(xr, ue1, ue3, ue2, *etab, max_tiles)
            part = _combine(y, ps, gt, *ctab)
            part, gatekeeper = lax.optimization_barrier((part, gatekeeper))
            ms.append(lax.psum_scatter(part, 'ep', scatter_dimension=0, tiled=True))
        m = jnp.concatenate(ms, axis=0)

        a = gatekeeper
        z = _rms(a, nf)
        hid = (jax.nn.silu(jnp.dot(z, w1, preferred_element_type=F32)) * jnp.dot(z, w3, preferred_element_type=F32)).astype(BF)
        af = a.astype(F32) + jnp.dot(hid, w2, preferred_element_type=F32)
        af, m = lax.optimization_barrier((af, m))
        return (af + m).astype(BF).reshape(b, s, d)

    rows_spec = P(('dp', 'ep'))
    in_specs = (rows_spec,) * 3 + (P(),) * 11 + (P('ep'),) * 3
    return jax.shard_map(local, mesh=mesh, in_specs=in_specs, out_specs=rows_spec, check_vma=False)
```

```python
import functools

import jax
import jax.numpy as jnp
from jax import lax
from jax.experimental import pallas as pl
from jax.experimental.pallas import tpu as pltpu
from jax.sharding import PartitionSpec as P

HEAD = 128
EPS = 1e-6
ROPE_BASE = 10000.0
CHUNKS = 2
GR = 8
BG = 320
BM = 320
TB = 128
WIN = 32
F32, BF = jnp.float32, jnp.bfloat16


def _rms(x, w):
    xf = x.astype(F32)
    r = lax.rsqrt(jnp.mean(xf * xf, axis=-1, keepdims=True) + EPS)
    return (xf * r * w.astype(F32)).astype(BF)


def _attn_kernel(scale, qb, q_ref, k_ref, v_ref, cos_ref, sin_ref, o_ref):
    cos, sin = cos_ref[...], sin_ref[...]
    half = HEAD // 2

    def rope(x):
        return (x * cos + pltpu.roll(x, half, 1) * sin).astype(BF)

    q, k, v = rope(q_ref[...]), rope(k_ref[...]), v_ref[...]
    n = q.shape[0] // qb
    row = lax.broadcasted_iota(jnp.int32, (qb, qb), 0)
    col = lax.broadcasted_iota(jnp.int32, (qb, qb), 1)
    dims = (((1,), (1,)), ((), ()))
    for i in range(n):
        qi = q[i * qb:(i + 1) * qb]
        kv = (i + 1) * qb
        diag = lax.dot_general(qi, k[i * qb:kv], dims, preferred_element_type=F32)
        s = jnp.where(row >= col, diag, -jnp.inf)
        if i:
            s = jnp.concatenate([lax.dot_general(qi, k[:i * qb], dims, preferred_element_type=F32), s], axis=1)
        p = jnp.exp((s - jnp.max(s, axis=-1, keepdims=True)) * scale)
        p = (p * (1.0 / jnp.sum(p, axis=-1, keepdims=True))).astype(BF)
        o = jnp.dot(p, v[:kv], preferred_element_type=F32)
        o_ref[i * qb:(i + 1) * qb, :] = o.astype(BF)


def _attention(q, k, v, cos, sin):
    s, dq = q.shape
    blk = pl.BlockSpec((s, HEAD), lambda h: (0, h))
    tab = pl.BlockSpec((s, HEAD), lambda h: (0, 0))
    return pl.pallas_call(
        functools.partial(_attn_kernel, HEAD ** -0.5, min(256, s)),
        out_shape=jax.ShapeDtypeStruct((s, dq), BF),
        grid=(dq // HEAD,),
        in_specs=[blk, blk, blk, tab, tab],
        out_specs=blk,
        compiler_params=pltpu.CompilerParams(vmem_limit_bytes=40 * 2**20),
        cost_estimate=pl.CostEstimate(flops=4 * s * s * dq, bytes_accessed=12 * s * dq, transcendentals=s * s * dq // HEAD),
        name="attention",
    )(q, k, v, cos, sin)


def _gather_kernel(ge, gr0, gdst, stot, u_ref, rk_ref, x_hbm, xbuf, sem, used):
    s = pl.program_id(0)
    tc = u_ref.shape[0]
    per = BG // GR
    iota = lax.broadcasted_iota(jnp.int32, (GR, tc), 0)

    @pl.when(s == 0)
    def _():
        used[0] = 0
        for slot in range(2):
            used[1 + 2 * slot] = 0
            used[2 + 2 * slot] = 1 << 20

    def copies(src, m, slot, act):
        for k in range(per):
            g = m * per + k

            @pl.when(g < stot[src])
            def _():
                act(pltpu.make_async_copy(
                    xbuf.at[slot, pl.ds(k * GR, GR), :],
                    x_hbm.at[pl.ds(pl.multiple_of(gdst[src, g] * GR, GR), GR), :],
                    sem.at[slot, k]))

    def drain(slot):
        copies(used[1 + 2 * slot], used[2 + 2 * slot], slot, lambda c: c.wait())

    def tile(m, _):
        slot = lax.rem(used[0], 2)
        parts = []
        for k in range(per):
            g = m * per + k
            row = rk_ref[0, pl.ds(ge[s, g], 1), :]
            parts.append(((iota + gr0[s, g]).astype(F32) == row).astype(F32))
        onehot = jnp.concatenate(parts, axis=0).astype(BF)
        x = jnp.dot(onehot, u_ref[...], preferred_element_type=F32).astype(BF)
        drain(slot)
        xbuf[slot] = x
        copies(s, m, slot, lambda c: c.start())
        used[1 + 2 * slot] = s
        used[2 + 2 * slot] = m
        used[0] += 1
        return 0

    lax.fori_loop(0, lax.div(stot[s] + per - 1, per), tile, 0)

    @pl.when(s == pl.num_programs(0) - 1)
    def _():
        drain(0)
        drain(1)


def _gather(u, rk, tabs, rows):
    srcs, el, tc = rk.shape
    d = u.shape[1]
    return pl.pallas_call(
        _gather_kernel,
        out_shape=jax.ShapeDtypeStruct((rows, d), BF),
        grid_spec=pltpu.PrefetchScalarGridSpec(
            num_scalar_prefetch=4,
            grid=(srcs,),
            in_specs=[pl.BlockSpec((tc, d), lambda s, *_: (s, 0)),
                      pl.BlockSpec((1, el, tc), lambda s, *_: (s, 0, 0))],
            out_specs=pl.BlockSpec(memory_space=pl.ANY),
            scratch_shapes=[pltpu.VMEM((2, BG, d), BF), pltpu.SemaphoreType.DMA((2, BG // GR)),
                            pltpu.SMEM((5,), jnp.int32)],
        ),
        compiler_params=pltpu.CompilerParams(vmem_limit_bytes=48 * 2**20),
        cost_estimate=pl.CostEstimate(flops=2 * rows * tc * d, bytes_accessed=4 * rows * d, transcendentals=0),
        name="gather_rows",
    )(*tabs, u, rk)


def _expert_kernel(tbase, tiles, tot, x_hbm, w1_ref, w3_ref, w2_ref, y_hbm, xbuf, ybuf, xsem, ysem):
    e = pl.program_id(0)
    last = pl.num_programs(0) - 1
    nt = tbase[last] + tiles[last]
    rows = lambda i: pl.ds(pl.multiple_of(i * BM, BM), BM)
    load = lambda i: pltpu.make_async_copy(x_hbm.at[rows(i), :], xbuf.at[lax.rem(i, 2)], xsem.at[lax.rem(i, 2)])
    save = lambda i: pltpu.make_async_copy(ybuf.at[lax.rem(i, 2)], y_hbm.at[rows(i), :], ysem.at[lax.rem(i, 2)])

    @pl.when(e == 0)
    def _():
        load(0).start()

    def tile(m, _):
        i = tbase[e] + m
        slot = lax.rem(i, 2)
        load(i).wait()

        @pl.when(i + 1 < nt)
        def _():
            load(i + 1).start()

        x = xbuf[slot]
        h1 = jnp.dot(x, w1_ref[0], preferred_element_type=F32)
        h3 = jnp.dot(x, w3_ref[0], preferred_element_type=F32)
        hid = (jax.nn.silu(h1) * h3).astype(BF)
        y = jnp.dot(hid, w2_ref[0], preferred_element_type=F32)
        row = lax.broadcasted_iota(jnp.int32, (BM, 1), 0)
        y = jnp.where(row < tot[e] - m * BM, y, 0.0).astype(BF)

        @pl.when(i >= 2)
        def _():
            save(i - 2).wait()

        ybuf[slot] = y
        save(i).start()
        return 0

    lax.fori_loop(0, tiles[e], tile, 0)

    @pl.when(e == last)
    def _():
        @pl.when(nt >= 2)
        def _():
            save(nt - 2).wait()

        save(nt - 1).wait()


def _experts(x, ue1, ue3, ue2, tbase, tiles, tot, max_tiles):
    el, d, fe = ue1.shape
    rows = max_tiles * BM
    wmap = lambda e, *_: (e, 0, 0)
    hbm = pl.BlockSpec(memory_space=pl.ANY)
    return pl.pallas_call(
        _expert_kernel,
        out_shape=jax.ShapeDtypeStruct((rows, d), BF),
        grid_spec=pltpu.PrefetchScalarGridSpec(
            num_scalar_prefetch=3,
            grid=(el,),
            in_specs=[hbm,
                      pl.BlockSpec((1, d, fe), wmap),
                      pl.BlockSpec((1, d, fe), wmap),
                      pl.BlockSpec((1, fe, d), wmap)],
            out_specs=hbm,
            scratch_shapes=[pltpu.VMEM((2, BM, d), BF), pltpu.VMEM((2, BM, d), BF),
                            pltpu.SemaphoreType.DMA((2,)), pltpu.SemaphoreType.DMA((2,))],
        ),
        compiler_params=pltpu.CompilerParams(vmem_limit_bytes=61 * 2**20),
        cost_estimate=pl.CostEstimate(flops=3 * rows * d * fe, bytes_accessed=6 * el * d * fe, transcendentals=rows * fe),
        name="experts",
    )(tbase, tiles, tot, x, ue1, ue3, ue2)


def _combine_kernel(nb, st, tend, nwin, y_hbm, pos_ref, g_ref, o_ref, ybuf, sem):
    s, b = pl.program_id(0), pl.program_id(1)
    el = pos_ref.shape[1]
    i = s * nb + b
    last = pl.num_programs(0) * nb - 1
    slot = lax.rem(i, 2)

    def start_of(step, e, w):
        return jnp.minimum(st[step, e] + w * WIN, tend[e] - WIN)

    def windows(step, w, sl, act):
        for e in range(el):
            act(pltpu.make_async_copy(
                y_hbm.at[pl.ds(pl.multiple_of(start_of(step, e, w), GR), WIN), :],
                ybuf.at[sl, pl.ds(e * WIN, WIN), :],
                sem.at[sl, e]))

    @pl.when(i == 0)
    def _():
        windows(0, 0, 0, lambda c: c.start())

    @pl.when(i < last)
    def _():
        windows(i + 1, 0, 1 - slot, lambda c: c.start())

    gates = g_ref[0]
    g1 = gates.astype(BF).astype(F32)
    r1 = gates - g1
    g2 = r1.astype(BF).astype(F32)
    terms = (g1, g2, r1 - g2)
    iota = lax.broadcasted_iota(jnp.int32, (WIN, TB), 0)

    def part(w, sl):
        cols = []
        for term in terms:
            rows = []
            for e in range(el):
                pos = pos_ref[0, e:e + 1, :]
                lo = st[i, e] + w * WIN
                ok = (pos >= lo) & (pos < lo + WIN)
                rel = jnp.where(ok, pos - start_of(i, e, w), -1)
                rows.append(jnp.where(iota == rel, term[e:e + 1, :], 0.0).astype(BF))
            cols.append(jnp.concatenate(rows, axis=0))
        wt = jnp.concatenate(cols, axis=1)
        r = lax.dot_general(wt, ybuf[sl], (((0,), (0,)), ((), ())), preferred_element_type=F32)
        return r[:TB] + r[TB:2 * TB] + r[2 * TB:]

    windows(i, 0, slot, lambda c: c.wait())
    o_ref[...] = part(0, slot)

    def more(w, _):
        windows(i, w, 2, lambda c: c.start())
        windows(i, w, 2, lambda c: c.wait())
        o_ref[...] += part(w, 2)
        return 0

    lax.fori_loop(1, nwin[i], more, 0)


def _combine(y, pos, gate, st, tend, nwin):
    srcs, el, tc = pos.shape
    d = y.shape[1]
    nb = tc // TB
    blk = pl.BlockSpec((1, el, TB), lambda s, b, *_: (s, 0, b))
    return pl.pallas_call(
        functools.partial(_combine_kernel, nb),
        out_shape=jax.ShapeDtypeStruct((srcs * tc, d), F32),
        grid_spec=pltpu.PrefetchScalarGridSpec(
            num_scalar_prefetch=3,
            grid=(srcs, nb),
            in_specs=[pl.BlockSpec(memory_space=pl.ANY), blk, blk],
            out_specs=pl.BlockSpec((TB, d), lambda s, b, *_: (s * nb + b, 0)),
            scratch_shapes=[pltpu.VMEM((3, el * WIN, d), BF), pltpu.SemaphoreType.DMA((3, el))],
        ),
        compiler_params=pltpu.CompilerParams(vmem_limit_bytes=48 * 2**20),
        cost_estimate=pl.CostEstimate(flops=6 * srcs * tc * el * WIN * d, bytes_accessed=4 * srcs * tc * d, transcendentals=0),
        name="combine",
    )(st, tend, nwin, y, pos, gate)


def _ffn_kernel(mb, z_ref, w1_ref, w3_ref, w2_ref, o_ref):
    j = pl.program_id(0)
    dims = (((1,), (1,)), ((), ()))

    def rows(m, _):
        at = pl.ds(pl.multiple_of(m * mb, mb), mb)
        z = z_ref[at, :]
        h1 = lax.dot_general(z, w1_ref[...], dims, preferred_element_type=F32)
        h3 = lax.dot_general(z, w3_ref[...], dims, preferred_element_type=F32)
        hid = (jax.nn.silu(h1) * h3).astype(BF)
        y = jnp.dot(hid, w2_ref[...], preferred_element_type=F32)

        @pl.when(j == 0)
        def _():
            o_ref[at, :] = y

        @pl.when(j > 0)
        def _():
            o_ref[at, :] += y

        return 0

    lax.fori_loop(0, z_ref.shape[0] // mb, rows, 0)


def _ffn(z, w1t, w3t, w2):
    t, d = z.shape
    ff = w2.shape[0]
    ft = max(n for n in range(16, 1300, 16) if ff % n == 0)
    one = pl.Buffered(1)
    wblk = pl.BlockSpec((ft, d), lambda j: (j, 0))
    return pl.pallas_call(
        functools.partial(_ffn_kernel, min(t, 512)),
        out_shape=jax.ShapeDtypeStruct((t, d), F32),
        grid=(ff // ft,),
        in_specs=[pl.BlockSpec((t, d), lambda j: (0, 0), pipeline_mode=one), wblk, wblk, wblk],
        out_specs=pl.BlockSpec((t, d), lambda j: (0, 0), pipeline_mode=one),
        compiler_params=pltpu.CompilerParams(vmem_limit_bytes=61 * 2**20),
        cost_estimate=pl.CostEstimate(flops=6 * t * d * ff, bytes_accessed=6 * d * ff, transcendentals=t * ff),
        name="ffn",
    )(z, w1t, w3t, w2)


def _final_kernel(per, a_ref, f_ref, *refs):
    i = pl.program_id(0)
    o_ref = refs[-1]
    for c, m_ref in enumerate(refs[:-1]):
        @pl.when(lax.div(i, per) == c)
        def _():
            o_ref[...] = (a_ref[...].astype(F32) + f_ref[...] + m_ref[...]).astype(BF)


def _final(a, f, ms):
    t, d = a.shape
    rb = TB
    per = ms[0].shape[0] // rb
    blk = pl.BlockSpec((rb, d), lambda i: (i, 0))
    mblk = [pl.BlockSpec((rb, d), lambda i, c=c: (jnp.clip(i - c * per, 0, per - 1), 0)) for c in range(len(ms))]
    return pl.pallas_call(
        functools.partial(_final_kernel, per),
        out_shape=jax.ShapeDtypeStruct((t, d), BF),
        grid=(t // rb,),
        in_specs=[blk, blk] + mblk,
        out_specs=blk,
        compiler_params=pltpu.CompilerParams(vmem_limit_bytes=32 * 2**20),
        cost_estimate=pl.CostEstimate(flops=2 * t * d, bytes_accessed=12 * t * d, transcendentals=0),
        name="final_sum",
    )(a, f, *ms)


def _excl(x, axis):
    return jnp.cumsum(x, axis=axis) - x


def _tables(rk, cap):
    srcs, el, tc = rk.shape
    i32 = jnp.int32
    nb = tc // TB
    has = (rk >= 0).reshape(srcs, el, nb, TB).sum(-1, dtype=i32)
    hi = jnp.cumsum(has, axis=2)
    lo = hi - has
    gran = (hi[:, :, -1] + GR - 1) // GR
    tot = gran.sum(0)
    tiles = jnp.maximum(1, (tot * GR + BM - 1) // BM)
    tbase = _excl(tiles, 0)
    seg = tbase * (BM // GR) + _excl(gran, 0)
    soff = _excl(gran, 1)
    stot = gran.sum(1)
    ng = el * (cap // GR + (cap % GR > 0)) + BG // GR
    gi = jnp.arange(ng, dtype=i32)
    own = (gi[None, :, None] >= soff[:, None, :]) & (gi[None, :, None] < (soff + gran)[:, None, :])
    eid = jnp.arange(el, dtype=i32)
    ge = jnp.sum(jnp.where(own, eid, 0), -1)
    live = gi[None, :] < stot[:, None]
    gr0 = jnp.where(live, gi[None, :] - jnp.sum(jnp.where(own, soff[:, None, :], 0), -1), 1 << 16) * GR
    gdst = jnp.sum(jnp.where(own, (seg - soff)[:, None, :], 0), -1) + gi[None, :]
    max_tiles = el * (-(-(srcs * (-(-cap // GR)) * GR) // BM))
    tend = (tbase + tiles) * BM
    lo16 = lo // GR * GR
    st = (lo16 + seg[:, :, None] * GR).transpose(0, 2, 1).reshape(srcs * nb, el)
    nwin = jnp.max((hi - lo16 + WIN - 1) // WIN, axis=1).reshape(srcs * nb)
    pos = jnp.where(rk >= 0, rk.astype(i32) + seg[:, :, None] * GR, -1)
    return (ge, gr0, gdst, stot), (tbase, tiles, tot * GR), (st, tend, nwin), pos, max_tiles


def solution(mesh):
    G = mesh.shape['ep']

    def local(h0, idx, slot, na, wq, wk, wv, wo, nf, w1, w3, w2, nm, wr, ue1, ue3, ue2):
        b, s, d = h0.shape
        t = b * s
        k = idx.shape[-1]
        el = ue1.shape[0]
        e = el * G
        cap = 2 * t * k // e
        tc = t // CHUNKS
        h = h0.reshape(t, d)

        u = _rms(h, nm)
        us = [lax.all_gather(u[c * tc:(c + 1) * tc], 'ep', axis=0, tiled=True) for c in range(CHUNKS)]

        idxt = idx.reshape(t, k).T
        hit = (idxt[:, None, :] == jnp.arange(e, dtype=jnp.int32)[None, :, None]).any(0)
        logits = lax.dot_general(wr, u, (((0,), (1,)), ((), ())), preferred_element_type=F32)
        top = jnp.max(jnp.where(hit, logits, -jnp.inf), axis=0, keepdims=True)
        ex = jnp.where(hit, jnp.exp(logits - top), 0.0)
        gate = ex / jnp.sum(ex, axis=0, keepdims=True)
        before = (jnp.arange(tc)[:, None] < jnp.arange(tc)[None, :]).astype(BF)
        rank = jnp.dot(hit.astype(BF).reshape(e * CHUNKS, tc), before, preferred_element_type=F32).reshape(e, t)
        rank = jnp.where(hit, rank, -1.0)
        route = jnp.concatenate([rank.reshape(G, el, t), gate.reshape(G, el, t)], axis=1)
        route = lax.all_to_all(route, 'ep', 0, 0, tiled=True)

        pos = jnp.arange(s).astype(F32)
        inv = ROPE_BASE ** (-2.0 * jnp.arange(HEAD // 2).astype(F32) / HEAD)
        ang = pos[:, None] * inv[None, :]
        cos, sin = jnp.cos(ang), jnp.sin(ang)
        cosf = jnp.concatenate([cos, cos], axis=1)
        sinf = jnp.concatenate([-sin, sin], axis=1)
        x = _rms(h, na)
        q = jnp.dot(x, wq, preferred_element_type=F32)
        kk = jnp.dot(x, wk, preferred_element_type=F32)
        v = jnp.dot(x, wv, preferred_element_type=F32).astype(BF)
        o = jnp.concatenate([_attention(q[i * s:(i + 1) * s], kk[i * s:(i + 1) * s], v[i * s:(i + 1) * s], cosf, sinf)
                             for i in range(b)], axis=0)
        a = (h.astype(F32) + jnp.dot(o, wo, preferred_element_type=F32)).astype(BF)

        ms = []
        gatekeeper = a
        for c in range(CHUNKS):
            rk = route[:, :el, c * tc:(c + 1) * tc]
            gt = route[:, el:, c * tc:(c + 1) * tc]
            gtab, etab, ctab, ps, max_tiles = _tables(rk, cap)
            uc, gatekeeper = lax.optimization_barrier((us[c], gatekeeper))
            xr = _gather(uc, rk, gtab, max_tiles * BM)
            y = _experts(xr, ue1, ue3, ue2, *etab, max_tiles)
            part = _combine(y, ps, gt, *ctab)
            part, gatekeeper = lax.optimization_barrier((part, gatekeeper))
            ms.append(lax.psum_scatter(part, 'ep', scatter_dimension=0, tiled=True))

        a = gatekeeper
        z = _rms(a, nf)
        f = _ffn(z, w1.T, w3.T, w2)
        return _final(a, f, ms).reshape(b, s, d)

    rows_spec = P(('dp', 'ep'))
    in_specs = (rows_spec,) * 3 + (P(),) * 11 + (P('ep'),) * 3
    return jax.shard_map(local, mesh=mesh, in_specs=in_specs, out_specs=rows_spec, check_vma=False)
```
